32 devices in a mesh: field: 4 (over x, core), slab: 8 (over z, y).
Axes of the slice: x: 2, y: 2, z: 4, core: 2. Of those that a mesh axis runs over, the one named last changes fastest.
Arguments:
- velocity_u: float32 [512, 512, 512], P('field', 'slab'), may hold values from -6 to 6
- velocity_v: float32 [512, 512, 512], P('field', 'slab'), may hold values from -6 to 6
- scalar_theta: float32 [512, 512, 512], P('field', 'slab'), may hold values from -6 to 6
Outputs:
- spectrum: float32 [4, 320, 320, 320], P('field', 'slab')
The draws below stay inside these ranges and needn't reach their ends.
All inputs are finite; a program needn't handle non-finite values.
Results may differ from the reference program's by a relative error of at most 0.00029.
Values sent between devices are 32-bit elements; how exact they have to be, the bound alone decides.
A program may use at most 256 MiB of HBM per device.

```python
import jax
import jax.numpy as jnp

N = 512
KEEP = 160


def levels(own_key, shape, cuts, smallest, largest):
    factor_of, own = 1.0, jax.random.fold_in(own_key, 6)
    for axis_at, parts in cuts:
        draws = jnp.exp(jax.random.uniform(jax.random.fold_in(own, axis_at), (parts,), jnp.float32, smallest / len(cuts), largest / len(cuts)))
        factor_of = factor_of * jnp.repeat(draws, shape[axis_at] // parts).reshape([-1 if axis == axis_at else 1 for axis in range(len(shape))])
    return factor_of


def gaussian(rng, extent, width, bound, pieces=(), held_as=jnp.bfloat16):
    entries = jax.random.normal(rng, extent, jnp.float32) * width
    if len(pieces) > 0:
        entries = levels(rng, extent, pieces, -0.22, 0.18) * entries
    return jnp.clip(entries, min=-bound, max=bound).astype(held_as)


def setup_inputs(seed: int = 0) -> dict:
    streams_of = jax.random.split(jax.random.key(seed), 4)
    return {
        "velocity_u": gaussian(streams_of[0], (N, N, N), 1.0, 6.0, ((0, 4), (1, 8)), jnp.float32),
        "velocity_v": gaussian(streams_of[1], (N, N, N), 1.0, 6.0, ((0, 4), (1, 8)), jnp.float32),
        "scalar_theta": gaussian(streams_of[2], (N, N, N), 1.0, 6.0, ((0, 4), (1, 8)), jnp.float32),
    }


def transform_one(field):
    scale = 1.0 / (N * jnp.sqrt(jnp.float32(N)))
    index = ((jnp.arange(2 * KEEP) - KEEP) % N).astype(jnp.int32)
    spec = jnp.fft.rfft(field, axis=2)[:, :, :KEEP]
    spec = jnp.fft.fft(spec, axis=0)[index]
    spec = jnp.fft.fft(spec, axis=1)[:, index]
    spec = spec * scale
    result = jnp.concatenate([jnp.real(spec), jnp.imag(spec)], axis=-1).astype(jnp.float32)
    return result.at[KEEP, KEEP, 0].set(0.0)

def reference(velocity_u, velocity_v, scalar_theta):
    outputs = [transform_one(velocity_u * velocity_u), transform_one(velocity_v * velocity_v), transform_one(velocity_u * velocity_v), transform_one(velocity_u * scalar_theta)]
    return jnp.stack(outputs, axis=0)
```

```python
import jax
import jax.numpy as jnp
from jax import lax
from jax.experimental import pallas as pl
from jax.experimental.pallas import tpu as pltpu
from jax.sharding import PartitionSpec as P

N = 512
KEEP = 160
CHUNKS = 8
KBLOCK = 4
HIGH = lax.Precision.HIGH


def waves_of(phase):
    angle = (phase % N).astype(jnp.float32) * (2.0 * jnp.pi / N)
    norm = 1.0 / jnp.sqrt(jnp.float32(N))
    return jnp.cos(angle) * norm, jnp.sin(angle) * norm


def depth_table():
    places = jnp.arange(N, dtype=jnp.int32)
    waves = jnp.arange(KEEP, dtype=jnp.int32)
    c, s = waves_of(places[:, None] * waves[None, :])
    return jnp.stack([c, -s], axis=0)


def complex_table(phase):
    c, s = waves_of(phase)
    return jnp.stack([jnp.stack([c, s]), jnp.stack([-s, c])])


def halves(x):
    high = x.astype(jnp.bfloat16)
    return high, (x - high.astype(jnp.float32)).astype(jnp.bfloat16)


def second_kernel(table_ref, piece_ref, *rest):
    out_ref = rest[-1]
    tables = [halves(table_ref[r]) for r in range(2)]
    for k in range(piece_ref.shape[0]):
        high, low = halves(piece_ref[k])
        for r in range(2):
            t_high, t_low = tables[r]
            value = jnp.dot(t_high, high, preferred_element_type=jnp.float32)
            value += jnp.dot(t_high, low, preferred_element_type=jnp.float32)
            value += jnp.dot(t_low, high, preferred_element_type=jnp.float32)
            cols = slice(r * KEEP, (r + 1) * KEEP)
            if len(rest) > 1:
                value += rest[0][k, :, cols]
            out_ref[k, :, cols] = value


def second(table, piece, total):
    rows, depth, _ = piece.shape
    wide = 2 * KEEP
    block = pl.BlockSpec((KBLOCK, wide, wide), lambda g: (g, 0, 0))
    specs = [
        pl.BlockSpec((2, wide, depth), lambda g: (0, 0, 0)),
        pl.BlockSpec((KBLOCK, depth, KEEP), lambda g: (g, 0, 0)),
    ]
    args = [table, piece]
    if total is not None:
        specs.append(block)
        args.append(total)
    return pl.pallas_call(
        second_kernel,
        out_shape=jax.ShapeDtypeStruct((rows, wide, wide), jnp.float32),
        grid=(rows // KBLOCK,),
        in_specs=specs,
        out_specs=block,
        input_output_aliases={2: 0} if total is not None else {},
        cost_estimate=pl.CostEstimate(
            flops=12 * rows * wide * depth * KEEP,
            bytes_accessed=4 * rows * (2 * wide * wide + depth * 256),
            transcendentals=0,
        ),
        compiler_params=pltpu.CompilerParams(vmem_limit_bytes=24 * 2**20),
    )(*args)


def make_shards(fields, slabs):
    def shards(u, v, t):
        f = lax.axis_index("field")
        xs, ys, _ = u.shape
        rows = 2 * KEEP // slabs
        step = ys // CHUNKS
        size = step * KEEP
        zt = depth_table()
        k = jnp.arange(2 * KEEP, dtype=jnp.int32) - KEEP
        rounds = jnp.arange(fields, dtype=jnp.int32)
        xg = ((f ^ rounds) * xs)[:, None] + jnp.arange(xs, dtype=jnp.int32)[None]
        xt = complex_table(k[:, None, None] * xg[None])
        xt = xt.reshape(2, 2, slabs, rows, fields, xs)
        yg = jnp.arange(N, dtype=jnp.int32)
        yt = complex_table(k[:, None] * yg[None]).reshape(2, 2, 2 * KEEP, slabs, CHUNKS, step)
        parts = []
        for i in range(CHUNKS):
            uc, vc, tc = (lax.slice_in_dim(a, i * step, (i + 1) * step, axis=1) for a in (u, v, t))
            got = []
            for m in range(fields):
                q = f ^ m
                left = jnp.where(q == 1, vc, uc)
                right = jnp.where(q == 0, uc, jnp.where(q == 3, tc, vc))
                part = jnp.einsum("xyz,rzc->rycx", left * right, zt, precision=HIGH)
                if m:
                    part = lax.ppermute(part, "field", [(a, a ^ m) for a in range(fields)])
                got.append(part)
            parts.append(got)
        total = None
        for i in range(CHUNKS):
            have = jnp.stack(parts[i], axis=0)
            mixed = jnp.einsum("RrSKmx,mrycx->SRKyc", xt, have, precision=HIGH)
            mixed = mixed.reshape(slabs, 2, rows, size)
            mixed = lax.all_to_all(mixed, "slab", split_axis=0, concat_axis=0, tiled=True)
            mixed = mixed.reshape(slabs, 2, rows, step, KEEP).transpose(2, 0, 1, 3, 4)
            mixed = mixed.reshape(rows, slabs * 2 * step, KEEP)
            table = yt[:, :, :, :, i].transpose(0, 2, 3, 1, 4).reshape(2, 2 * KEEP, -1)
            total = second(table, mixed, total)
        row = KEEP - lax.axis_index("slab") * rows
        mine = (row >= 0) & (row < rows)
        at = (0, jnp.clip(row, 0, rows - 1), KEEP, 0)
        total = total[None]
        old = lax.dynamic_slice(total, at, (1, 1, 1, 1))
        return lax.dynamic_update_slice(total, jnp.where(mine, jnp.float32(0.0), old), at)

    return shards


def solution(mesh):
    spec = P("field", "slab", None)
    fields = mesh.shape["field"]
    return jax.shard_map(
        make_shards(fields, mesh.shape["slab"]),
        mesh=mesh,
        in_specs=(spec, spec, spec),
        out_specs=P("field", "slab", None, None),
        check_vma=False,
    )
```
